1024 devices in a mesh: section: 128 (over y, x, z_lo), tp: 8 (over z_hi, core).
Axes of the slice: x: 8, y: 8, z: 8 (z_hi: 4, z_lo: 2; z = z_hi * 2 + z_lo), core: 2. Of those that a mesh axis runs over, the one named last changes fastest.
Arguments:
- stash: bfloat16 [128, 2, 512, 4096], P('section', None, 'tp'), may hold values from -660 to 660
- slot: int32 [128], P('section'), may hold values from 0 to 1
- doc_ids: int32 [128, 2, 512], P('section', None, 'tp'), may hold values from 0 to 3, never falling along the last dimension, each value on 1 to 256 neighbouring positions
- norm_gain: bfloat16 [4096], replicated, may hold values from 0.099609375 to 1.8984375
- w_query: bfloat16 [4096, 4096], P(None, 'tp'), may hold values from -21 to 21
- w_key: bfloat16 [4096, 1024], P(None, 'tp'), may hold values from -21 to 21
- value_weight: bfloat16 [4096, 1024], P(None, 'tp'), may hold values from -0.09375 to 0.09375
Outputs:
- received: bfloat16 [128, 512, 4096], P('section', None, 'tp')
The draws below stay inside these ranges and needn't reach their ends.
Inputs may be any that keep to these rules, and one draw needn't show every extreme that they name: `doc_ids`: document numbers never fall along a micro-batch.
All inputs are finite; a program needn't handle non-finite values.
Results may differ from the reference program's by a relative error of at most 0.025.
The reference program's roundings to bfloat16 on the way (of `picked`, `normed`, `values`, `softmax_weights` and `context`) count: a program that leaves them out, or rounds other values in their place, can miss the bound.
Values may be sent and summed in bfloat16 or wider, within the bound.
No kernel may reach another device: no remote copies, remote signals or barrier semaphores. Data moves between devices by JAX's collectives and lax.ppermute only.
A program may use at most 64 MiB of HBM per device.

```python
import math
import jax
import jax.numpy as jnp
import numpy as np
from jax import lax

MODEL_WIDTH = 4096
HQ = 32
VALUE_KEY_HEADS = 8
HEAD_SIZE = 128
SLOTS = 2
DOCS = 4
TOK = 512
SECTIONS = 128


def weight_with_spike(key, salt_value, columns):
    gaussian = jax.random.truncated_normal(jax.random.fold_in(key, salt_value), -4.0, 4.0, (MODEL_WIDTH, columns), jnp.float32)
    gaussian = gaussian / jnp.sqrt(jnp.float32(MODEL_WIDTH))
    return gaussian.astype(jnp.bfloat16)


def draw_w_query(key, part):
    return weight_with_spike(key, 1, HQ * HEAD_SIZE)


def draw_w_key(key, part):
    return weight_with_spike(key, 2, VALUE_KEY_HEADS * HEAD_SIZE)


def draw_stash(key, part):
    full_shape = (SECTIONS, SLOTS, TOK, MODEL_WIDTH)
    col_scale = jnp.exp(jax.random.uniform(jax.random.fold_in(key, 12), (MODEL_WIDTH,), jnp.float32, 0.0, math.log(10.0)))
    row_scale = jnp.exp(jax.random.uniform(jax.random.fold_in(key, 11), (SECTIONS, SLOTS, TOK, 1), jnp.float32, 0.0, math.log(10.0)))
    noise_part = jax.random.truncated_normal(jax.random.fold_in(key, 13), -4.0, 4.0, full_shape, jnp.float32)
    result = noise_part * row_scale * col_scale
    return result.astype(jnp.bfloat16)


def place_ends(values, rng, low, largest):
    dims = values.shape
    spot = [jax.random.randint(jax.random.fold_in(rng, axis), (), 0, dims[axis]) for axis in range(len(dims))]
    values = values.at[tuple(spot)].set(low)
    longest = dims.index(max(dims))
    spot[longest] = (spot[longest] + 1) % dims[longest]
    return values.at[tuple(spot)].set(largest)


def block_levels(key, extent, cuts, least, largest):
    level, own = 1.0, jax.random.fold_in(key, 6)
    for position, shards_of in cuts:
        steps = jnp.exp(jax.random.uniform(jax.random.fold_in(own, position), (shards_of,), jnp.float32, least / len(cuts), largest / len(cuts)))
        level = level * jnp.repeat(steps, extent[position] // shards_of).reshape([-1 if axis == position else 1 for axis in range(len(extent))])
    return level


def length_profile(amount, total, bound, slope):
    loads = [(1 << 20) // math.isqrt(grade ** slope) + 1 for grade in range(2, amount + 1)]
    rest, holding = total - bound - (amount - 1), [1] * (amount - 1)
    while rest > 0:
        movable = [i for i in range(amount - 1) if holding[i] < bound]
        mass, remaining = sum([loads[i] for i in movable]), rest
        for i in movable:
            extra = min(bound - holding[i], max(1, remaining * loads[i] // mass), rest)
            holding[i] = holding[i] + extra
            rest = rest - extra
    return np.array([bound] + holding)


def ragged(key, count, total, most, lean):
    if count == 2:
        one = jax.random.randint(key, (), max(1, total - most), min(most, total - 1) + 1)
        return jnp.stack([one, total - one])
    tallies = jnp.asarray(length_profile(count, total, most, lean), jnp.int32)
    pairs = (count - 1) // 2
    donor, receiver = tallies[1:1 + 2 * pairs:2], tallies[2:2 + 2 * pairs:2]
    slack = jnp.minimum(donor - 1, most - receiver)
    moved = jax.random.randint(jax.random.fold_in(key, 1), (pairs,), 0, 1 << 20) % (slack + 1)
    tallies = tallies.at[1:1 + 2 * pairs:2].set(donor - moved).at[2:2 + 2 * pairs:2].set(receiver + moved)
    return tallies[jax.random.permutation(jax.random.fold_in(key, 2), count)]


def noise(stream_key, extent, width, most, split=(), kind=jnp.bfloat16):
    entries = jax.random.normal(stream_key, extent, jnp.float32) * width
    if len(split) > 0:
        entries = block_levels(stream_key, extent, split, -0.22, 0.18) * entries
    return jnp.clip(entries, min=-most, max=most).astype(kind)


def setup_inputs(seed: int = 0) -> dict:
    splits = jax.random.split(jax.random.key(seed), 8)
    stash = draw_stash(jax.random.fold_in(splits[7], 71), 0)
    slot = place_ends(jax.random.randint(splits[1], (SECTIONS,), 0, SLOTS), jax.random.fold_in(splits[1], 1), 0, SLOTS - 1).astype(jnp.int32)
    doc_ids = jax.vmap(lambda own: jnp.searchsorted(jnp.cumsum(ragged(own, DOCS, TOK, TOK // 2, 1)), jnp.arange(TOK), side="right"))(jax.random.split(splits[2], SECTIONS * SLOTS)).reshape((SECTIONS, SLOTS, TOK)).astype(jnp.int32)
    norm_gain = jnp.clip(1.0 + 0.18 * jax.random.normal(splits[3], (MODEL_WIDTH,), jnp.float32), 0.099609375, 1.8984375).astype(jnp.bfloat16)
    w_query = draw_w_query(jax.random.fold_in(splits[7], 71), 0)
    w_key = draw_w_key(jax.random.fold_in(splits[7], 71), 0)
    value_weight = noise(splits[6], (MODEL_WIDTH, VALUE_KEY_HEADS * HEAD_SIZE), MODEL_WIDTH ** -0.5, 0.09375, ((1, 8),))
    return dict(stash=stash, slot=slot, doc_ids=doc_ids, norm_gain=norm_gain, w_query=w_query, w_key=w_key, value_weight=value_weight)


ROPE_BASE = 500000.0
NORM_EPSILON = 1e-05

def rotate(values, positions):
    head_width = values.shape[-1]
    half_width = head_width // 2
    freq_index = jnp.arange(half_width, dtype=jnp.float32)
    inverse = jnp.power(jnp.float32(ROPE_BASE), -2.0 * freq_index / head_width)
    angles = positions.astype(jnp.float32)[:, None] * inverse[None, :]
    cosine = jnp.concatenate([jnp.cos(angles), jnp.cos(angles)], -1)[:, None, :]
    sine_part = jnp.concatenate([jnp.sin(angles), jnp.sin(angles)], -1)[:, None, :]
    turned = jnp.concatenate([-values[..., half_width:], values[..., :half_width]], -1)
    return values * cosine + turned * sine_part

def normalize(stash_rows, norm_gain):
    widened = stash_rows.astype(jnp.float32)
    mean_square = lax.optimization_barrier(jnp.mean(widened * widened, axis=-1, keepdims=True))
    return (widened * lax.rsqrt(mean_square + NORM_EPSILON) * norm_gain.astype(jnp.float32)).astype(jnp.bfloat16)

def project(normed, weight, positions, use_rope):
    length = normed.shape[0]
    product = jnp.dot(normed, weight, preferred_element_type=jnp.float32)
    if use_rope:
        product = rotate(product.reshape(length, -1, HEAD_SIZE), positions).reshape(length, -1)
    return product.astype(jnp.bfloat16)

def attend(queries, keys, values, doc_rows):
    length = queries.shape[0]
    kv_count = keys.shape[1] // HEAD_SIZE
    group_size = queries.shape[1] // HEAD_SIZE // kv_count
    grouped = queries.astype(jnp.float32).reshape(length, kv_count, group_size, HEAD_SIZE)
    key_heads = keys.astype(jnp.float32).reshape(length, kv_count, HEAD_SIZE)
    value_heads = values.astype(jnp.float32).reshape(length, kv_count, HEAD_SIZE)
    scores = jnp.einsum('ihgd,jhd->hgij', grouped, key_heads) * (1.0 / math.sqrt(HEAD_SIZE))
    row_index = jnp.arange(length, dtype=jnp.int32)[:, None]
    col_index = jnp.arange(length, dtype=jnp.int32)[None, :]
    allowed = (col_index <= row_index) & (doc_rows[None, :] == doc_rows[:, None])
    scores = jnp.where(allowed, scores, -1e+30)
    row_max = lax.optimization_barrier(jnp.max(scores, axis=-1, keepdims=True))
    score_exponent = jnp.exp(scores - row_max)
    softmax_weights = (score_exponent / lax.optimization_barrier(jnp.sum(score_exponent, axis=-1, keepdims=True))).astype(jnp.bfloat16)
    context = jnp.einsum('hgij,jhd->ihgd', softmax_weights.astype(jnp.float32), value_heads)
    return context.reshape(length, -1).astype(jnp.bfloat16)

def reference(stash, slot, doc_ids, norm_gain, w_query, w_key, value_weight):
    positions = jnp.arange(TOK, dtype=jnp.int32)

    def one_section(inputs):
        section_stash, section_slot, section_docs = inputs
        picked = lax.dynamic_index_in_dim(section_stash, section_slot, 0, keepdims=False)
        doc_rows = lax.dynamic_index_in_dim(section_docs, section_slot, 0, keepdims=False)
        normed = normalize(picked, norm_gain)
        queries = project(normed, w_query, positions, True)
        keys = project(normed, w_key, positions, True)
        values = project(normed, value_weight, positions, False)
        return attend(queries, keys, values, doc_rows)
    context_rows = lax.map(one_section, (stash, slot, doc_ids))
    return jnp.concatenate([jnp.zeros_like(context_rows[:1]), context_rows[:-1]], 0)
```

```python
import functools
import math

import jax
import jax.numpy as jnp
from jax import lax
from jax.experimental import pallas as pl
from jax.experimental.pallas import tpu as pltpu
from jax.sharding import PartitionSpec as P

HEAD_SIZE = 128
LANES = 128
ROPE_BASE = 500000.0
NORM_EPSILON = 1e-05
AXES = ("section", "tp")
VMEM = pltpu.MemorySpace.VMEM


def normalize_kernel(slot_ref, stash_ref, doc_ref, gain_ref, out_ref, buf, sems):
    rows, width = buf.shape
    pieces = sems.shape[0]
    step = rows // pieces
    slot = slot_ref[0]

    def piece(i):
        part = pl.ds(i * step, step)
        return pltpu.make_async_copy(stash_ref.at[0, slot, part], buf.at[part], sems.at[i])

    for i in range(pieces):
        piece(i).start()
    docs = doc_ref[0, pl.ds(slot, 1), :].astype(jnp.float32)
    row = lax.broadcasted_iota(jnp.int32, (rows, rows), 0)
    column = lax.broadcasted_iota(jnp.int32, (rows, rows), 1)
    upright = jnp.sum(jnp.where(row == column, docs, 0.0), axis=1, keepdims=True)
    out_ref[:, width:] = jnp.broadcast_to(upright, (rows, LANES)).astype(jnp.bfloat16)
    gain = gain_ref[...].astype(jnp.float32)
    for i in range(pieces):
        piece(i).wait()
        part = slice(i * step, (i + 1) * step)
        x = buf[part, :].astype(jnp.float32)
        mean_square = jnp.mean(x * x, axis=-1, keepdims=True)
        scaled = x * lax.rsqrt(mean_square + NORM_EPSILON)
        out_ref[part, :width] = (scaled * gain).astype(jnp.bfloat16)


def normalize(slot, stash, doc_ids, gain):
    rows, width = stash.shape[2:]
    pieces = 4
    return pl.pallas_call(
        normalize_kernel,
        out_shape=jax.ShapeDtypeStruct((rows, width + LANES), jnp.bfloat16),
        in_specs=[
            pl.BlockSpec(memory_space=pltpu.MemorySpace.SMEM),
            pl.BlockSpec(memory_space=pltpu.MemorySpace.HBM),
            pl.BlockSpec(memory_space=VMEM),
            pl.BlockSpec(memory_space=VMEM),
        ],
        out_specs=pl.BlockSpec(memory_space=VMEM),
        scratch_shapes=[
            pltpu.VMEM((rows, width), jnp.bfloat16),
            pltpu.SemaphoreType.DMA((pieces,)),
        ],
        compiler_params=pltpu.CompilerParams(vmem_limit_bytes=4 << 20),
    )(slot, stash, doc_ids, gain.reshape(1, -1))


def project_blocks(blocks, weights):
    w_query, w_key, w_value = weights
    width = w_query.shape[0]
    x = jnp.concatenate([block[:, :width] for block in blocks], axis=0)
    results = []
    for start in range(0, w_query.shape[1], 256):
        w = w_query[:, start : start + 256]
        results.append(jnp.dot(x, w, preferred_element_type=jnp.float32))
    w = jnp.concatenate([w_key[...], w_value[...]], axis=1)
    results.append(jnp.dot(x, w, preferred_element_type=jnp.float32))
    return results


def turn_and_store(products, granules, cosine, sine, store):
    rows = products[0].shape[0] // len(granules)
    for index, granule in enumerate(granules):
        at = pl.ds(pl.multiple_of(granule * rows, rows), rows)
        cos, sin = cosine[at, :], sine[at, :]
        column = 0
        for number, product in enumerate(products):
            for half in range(2):
                values = product[index * rows : (index + 1) * rows, half * 128 : half * 128 + 128]
                if not (number == len(products) - 1 and half == 1):
                    values = values * cos + pltpu.roll(values, 64, 1) * sin
                store(index, at, column, values.astype(jnp.bfloat16))
                column += 128


def project_kernel(granules_ref, b0, b1, b2, b3, w_query, w_key, w_value, cosine, sine, out_ref):
    blocks = (b0, b1, b2, b3)
    products = project_blocks(blocks, (w_query, w_key, w_value))
    rows = b0.shape[0]
    width = w_query.shape[0]

    def store(index, at, column, values):
        out_ref[index * rows : (index + 1) * rows, column : column + 128] = values

    turn_and_store(products, [granules_ref[i] for i in range(4)], cosine, sine, store)
    for index, block in enumerate(blocks):
        out_ref[index * rows : (index + 1) * rows, 768:] = block[:, width:]


def project(granules, blocks, weights, cosine, sine):
    rows = blocks[0].shape[0]
    vmem = pl.BlockSpec(memory_space=VMEM)
    flops = 2 * 4 * rows * weights[0].shape[0] * 768
    return pl.pallas_call(
        project_kernel,
        out_shape=jax.ShapeDtypeStruct((4 * rows, 768 + LANES), jnp.bfloat16),
        in_specs=[pl.BlockSpec(memory_space=pltpu.MemorySpace.SMEM)] + [vmem] * 9,
        out_specs=vmem,
        compiler_params=pltpu.CompilerParams(vmem_limit_bytes=20 << 20),
        cost_estimate=pl.CostEstimate(flops=flops, bytes_accessed=10 << 20, transcendentals=0),
    )(granules, *blocks, *weights, cosine, sine)


def attend_kernel(
    granules_ref, early, b0, b1, b2, b3, w_query, w_key, w_value, cosine, sine, out_ref, rows_ref
):
    blocks = (b0, b1, b2, b3)
    rows = b0.shape[0]
    width = w_query.shape[0]
    products = project_blocks(blocks, (w_query, w_key, w_value))
    for index in range(4):
        at = pl.ds(pl.multiple_of(granules_ref[index] * rows, rows), rows)
        rows_ref[at, :] = early[index * rows : (index + 1) * rows, :]

    def store(index, at, column, values):
        rows_ref[at, column : column + 128] = values

    late = [granules_ref[4 + i] for i in range(4)]
    turn_and_store(products, late, cosine, sine, store)
    for index, block in enumerate(blocks):
        at = pl.ds(pl.multiple_of(late[index] * rows, rows), rows)
        rows_ref[at, 768:] = block[:, width:]

    total = rows_ref.shape[0]
    heads = 4
    tile = 128
    factor = math.log2(math.e) / math.sqrt(HEAD_SIZE)
    contract_last = (((1,), (1,)), ((), ()))
    ones = jnp.ones((8, LANES), jnp.bfloat16)
    lying = lax.dot_general(
        ones, rows_ref[:, 768:], contract_last, preferred_element_type=jnp.float32
    )[:1, :]
    for i in range(total // tile):
        seen = (i + 1) * tile
        here = slice(i * tile, seen)
        upright = rows_ref[here, 768:769].astype(jnp.float32) * float(LANES)
        row = lax.broadcasted_iota(jnp.int32, (tile, seen), 0) + i * tile
        column = lax.broadcasted_iota(jnp.int32, (tile, seen), 1)
        allowed = (column <= row) & (lying[:, :seen] == upright)
        bias = jnp.where(allowed, 0.0, -1e30)
        keys = rows_ref[:seen, 512:640]
        values = rows_ref[:seen, 640:768]
        for head in range(heads):
            lanes = slice(head * 128, (head + 1) * 128)
            scores = lax.dot_general(
                rows_ref[here, lanes], keys, contract_last, preferred_element_type=jnp.float32
            )
            scores = scores + bias
            row_max = jnp.max(scores, axis=-1, keepdims=True)
            exponent = jnp.exp2((scores - row_max) * factor)
            row_sum = jnp.sum(exponent, axis=-1, keepdims=True)
            context = jnp.dot(
                exponent.astype(jnp.bfloat16), values, preferred_element_type=jnp.float32
            )
            out_ref[0, here, lanes] = (context / row_sum).astype(jnp.bfloat16)


def attend(granules, early, blocks, weights, cosine, sine):
    rows = blocks[0].shape[0]
    vmem = pl.BlockSpec(memory_space=VMEM)
    flops = 2 * 4 * rows * weights[0].shape[0] * 768
    return pl.pallas_call(
        attend_kernel,
        out_shape=jax.ShapeDtypeStruct((1, 8 * rows, weights[0].shape[1]), jnp.bfloat16),
        in_specs=[pl.BlockSpec(memory_space=pltpu.MemorySpace.SMEM)] + [vmem] * 10,
        out_specs=vmem,
        scratch_shapes=[pltpu.VMEM((8 * rows, 768 + LANES), jnp.bfloat16)],
        compiler_params=pltpu.CompilerParams(vmem_limit_bytes=20 << 20),
        cost_estimate=pl.CostEstimate(flops=2 * flops, bytes_accessed=10 << 20, transcendentals=0),
    )(granules, early, *blocks, *weights, cosine, sine)


def routes(sections, group):
    def place(section, t):
        return section * group + t % group

    first, second, sibling = [], [], []
    for s in range(sections):
        for t in range(group):
            up = t % 2 == 0
            if s + 1 < sections:
                shift = (2 if up else 0) if s % 2 else (0 if up else -2)
                first.append((place(s, t), place(s + 1, t + shift)))
            second.append((place(s, t), place(s, t + (2 if up else -2))))
            sibling.append((place(s, t), place(s, t ^ 1)))
    return first, second, sibling


def per_device(sections, group, stash, slot, doc_ids, norm_gain, w_query, w_key, value_weight):
    first, second, sibling = routes(sections, group)

    def go(block, route):
        return lax.ppermute(block, AXES, route)

    own = normalize(slot, stash, doc_ids, norm_gain)
    other = go(own, sibling)
    near_a, near_b = go(own, first), go(other, first)
    far_a, far_b = go(near_a, second), go(near_b, second)
    near_c, near_d = go(near_a, sibling), go(near_b, sibling)
    far_c, far_d = go(far_a, sibling), go(far_b, sibling)

    total = stash.shape[2] * group
    positions = jnp.arange(total, dtype=jnp.int32)
    freq_index = jnp.arange(HEAD_SIZE // 2, dtype=jnp.float32)
    inverse = jnp.power(jnp.float32(ROPE_BASE), -2.0 * freq_index / HEAD_SIZE)
    angles = positions.astype(jnp.float32)[:, None] * inverse[None, :]
    cosine = jnp.concatenate([jnp.cos(angles), jnp.cos(angles)], -1)
    sine = jnp.concatenate([-jnp.sin(angles), jnp.sin(angles)], -1)

    t = lax.axis_index("tp")
    z_hi, core = t // 2, t % 2
    odd = 1 - lax.axis_index("section") % 2
    chips = group // 2
    base = z_hi - odd + chips
    mine = jnp.where(core == 0, jnp.stack([base, base - 1]), jnp.stack([base + 1, base + 2]))
    theirs = jnp.where(core == 0, jnp.stack([base + 1, base + 2]), jnp.stack([base, base - 1]))
    mine, theirs = 2 * (mine % chips), 2 * (theirs % chips)
    granules = jnp.stack(
        [
            mine[0] + core,
            mine[0] + 1 - core,
            theirs[0] + 1 - core,
            theirs[0] + core,
            mine[1] + core,
            mine[1] + 1 - core,
            theirs[1] + 1 - core,
            theirs[1] + core,
        ]
    ).astype(jnp.int32)
    weights = (w_query, w_key, value_weight)
    early = project(granules, (near_a, near_b, near_c, near_d), weights, cosine, sine)
    return attend(granules, early, (far_a, far_b, far_c, far_d), weights, cosine, sine)


def solution(mesh):
    placed = (
        P("section", None, "tp", None),
        P("section"),
        P("section", None, "tp"),
        P(),
        P(None, "tp"),
        P(None, "tp"),
        P(None, "tp"),
    )
    return jax.shard_map(
        functools.partial(per_device, mesh.shape["section"], mesh.shape["tp"]),
        mesh=mesh,
        in_specs=placed,
        out_specs=P("section", None, "tp"),
        check_vma=False,
    )
```

```python
import functools
import math

import jax
import jax.numpy as jnp
import numpy as np
from jax import lax
from jax.experimental import pallas as pl
from jax.experimental.pallas import tpu as pltpu
from jax.sharding import PartitionSpec as P

HEAD_SIZE = 128
LANES = 128
ROPE_BASE = 500000.0
NORM_EPSILON = 1e-05
AXES = ("section", "tp")
VMEM = pltpu.MemorySpace.VMEM


def fetch(source, target, sem):
    return pltpu.make_async_copy(source, target, sem)


def normalize_kernel(
    slot_ref, stash_ref, doc_ref, gain_ref, out_ref, docs, gain_buf, buf, sems
):
    rows, width = buf.shape
    pieces = sems.shape[0] - 2
    step = rows // pieces
    pick = slot_ref[0]
    copies = [
        fetch(doc_ref, docs, sems.at[0]),
        fetch(gain_ref, gain_buf, sems.at[1]),
    ]
    for i in range(pieces):
        part = pl.ds(i * step, step)
        copies.append(fetch(stash_ref.at[0, pick, part], buf.at[part], sems.at[2 + i]))
    for copy in copies:
        copy.start()
    for copy in copies[:2]:
        copy.wait()
    numbers = docs[0, pl.ds(pick, 1), :].astype(jnp.float32)
    row = lax.broadcasted_iota(jnp.int32, (rows, rows), 0)
    column = lax.broadcasted_iota(jnp.int32, (rows, rows), 1)
    upright = jnp.sum(jnp.where(row == column, numbers, 0.0), axis=1, keepdims=True)
    out_ref[:, width:] = jnp.broadcast_to(upright, (rows, LANES)).astype(jnp.bfloat16)
    gain = gain_buf[...].astype(jnp.float32)
    for i in range(pieces):
        copies[2 + i].wait()
        part = slice(i * step, (i + 1) * step)
        x = buf[part, :].astype(jnp.float32)
        scale = lax.rsqrt(jnp.mean(x * x, axis=-1, keepdims=True) + NORM_EPSILON)
        for j in range(width // LANES):
            lanes = slice(j * LANES, (j + 1) * LANES)
            scaled = x[:, lanes] * scale * gain[j : j + 1, :]
            out_ref[part, lanes] = scaled.astype(jnp.bfloat16)


def normalize(slot, stash, doc_ids, gain):
    rows, width = stash.shape[2:]
    pieces = 4
    hbm = pl.BlockSpec(memory_space=pltpu.MemorySpace.HBM)

    def stay(x):
        return pltpu.with_memory_space_constraint(x, pltpu.MemorySpace.HBM)

    return pl.pallas_call(
        normalize_kernel,
        out_shape=jax.ShapeDtypeStruct((rows, width + LANES), jnp.bfloat16),
        in_specs=[pl.BlockSpec(memory_space=pltpu.MemorySpace.SMEM)] + [hbm] * 3,
        out_specs=pl.BlockSpec(memory_space=VMEM),
        scratch_shapes=[
            pltpu.VMEM(doc_ids.shape, doc_ids.dtype),
            pltpu.VMEM((width // LANES, LANES), gain.dtype),
            pltpu.VMEM((rows, width), jnp.bfloat16),
            pltpu.SemaphoreType.DMA((2 + pieces,)),
        ],
        compiler_params=pltpu.CompilerParams(vmem_limit_bytes=8 << 20),
    )(slot, stay(stash), stay(doc_ids), stay(gain.reshape(-1, LANES)))


def tables_kernel(inverse_ref, cosine, sine):
    rows = cosine.shape[0]
    position = lax.broadcasted_iota(jnp.int32, (rows, LANES), 0).astype(jnp.float32)
    lane = lax.broadcasted_iota(jnp.int32, (rows, LANES), 1)
    angle = position * inverse_ref[...]
    cosine[...] = jnp.cos(angle)
    turned = jnp.sin(angle)
    sine[...] = jnp.where(lane < HEAD_SIZE // 2, -turned, turned)


def tables(total):
    exponent = -2.0 * np.arange(HEAD_SIZE // 2) / HEAD_SIZE
    inverse = np.tile(ROPE_BASE**exponent, 2)[None].astype(np.float32)
    vmem = pl.BlockSpec(memory_space=VMEM)
    shape = jax.ShapeDtypeStruct((total, LANES), jnp.float32)
    return pl.pallas_call(
        tables_kernel,
        out_shape=(shape, shape),
        in_specs=[vmem],
        out_specs=(vmem, vmem),
        compiler_params=pltpu.CompilerParams(vmem_limit_bytes=8 << 20),
        cost_estimate=pl.CostEstimate(flops=4 << 20, bytes_accessed=1 << 20, transcendentals=0),
    )(inverse)


def granule(chip_shift, mine, swapped):
    t, odd = lax.axis_index("tp"), 1 - lax.axis_index("section") % 2
    core, chips = t % 2, lax.axis_size("tp") // 2
    up = core if mine else 1 - core
    chip = lax.rem(t // 2 - odd + chips + jnp.where(up == 0, -chip_shift, 1 + chip_shift), chips)
    return 2 * chip + (1 - up if swapped else up)


def project_to(pieces, weights, cosine, sine, store):
    w_query, w_key, w_value = weights
    width = w_query.shape[0]
    rows = pieces[0][0].shape[0]
    x = jnp.concatenate([block[:, :width] for block, _ in pieces], axis=0)
    w_both = jnp.concatenate([w_key[...], w_value[...]], axis=1)
    products = [
        jnp.dot(x, w, preferred_element_type=jnp.float32)
        for w in (w_query[:, :256], w_query[:, 256:], w_both)
    ]
    for index, (block, number) in enumerate(pieces):
        at = pl.ds(pl.multiple_of(number * rows, rows), rows)
        cos, sin = cosine[at, :], sine[at, :]
        for head in range(6):
            values = products[head // 2][index * rows : (index + 1) * rows]
            values = values[:, (head % 2) * 128 : (head % 2) * 128 + 128]
            if head < 5:
                values = values * cos + pltpu.roll(values, 64, 1) * sin
            store(index, at, head * 128, values.astype(jnp.bfloat16))
        store(index, at, 768, block[:, width:])


def project_kernel(where, b0, b1, w_query, w_key, w_value, cosine, sine, out_ref):
    rows = b0.shape[0]

    def store(index, at, column, values):
        out_ref[index * rows : (index + 1) * rows, column : column + 128] = values

    pieces = [(block, granule(*place)) for block, place in zip((b0, b1), where)]
    project_to(pieces, (w_query, w_key, w_value), cosine, sine, store)


def project(where, blocks, weights, cosine, sine):
    rows = blocks[0].shape[0]
    vmem = pl.BlockSpec(memory_space=VMEM)
    flops = 2 * 2 * rows * weights[0].shape[0] * 768
    return pl.pallas_call(
        functools.partial(project_kernel, where),
        out_shape=jax.ShapeDtypeStruct((2 * rows, 768 + LANES), jnp.bfloat16),
        in_specs=[vmem] * 7,
        out_specs=vmem,
        compiler_params=pltpu.CompilerParams(vmem_limit_bytes=16 << 20),
        cost_estimate=pl.CostEstimate(flops=flops, bytes_accessed=8 << 20, transcendentals=0),
    )(*blocks, *weights, cosine, sine)


def attend_kernel(
    where, e0, e1, e2, b0, b1, w_query, w_key, w_value, cosine, sine, out_ref, rows_ref
):
    rows = b0.shape[0]

    def store(index, at, column, values):
        rows_ref[at, column : column + 128] = values

    for pair, early in zip(where, (e0, e1, e2)):
        for index, place in enumerate(pair):
            at = pl.ds(pl.multiple_of(granule(*place) * rows, rows), rows)
            rows_ref[at, :] = early[index * rows : (index + 1) * rows, :]
    pieces = [(block, granule(*place)) for block, place in zip((b0, b1), where[3])]
    project_to(pieces, (w_query, w_key, w_value), cosine, sine, store)

    total = rows_ref.shape[0]
    heads, tile = 4, 128
    factor = math.log2(math.e) / math.sqrt(HEAD_SIZE)
    contract_last = (((1,), (1,)), ((), ()))
    ones = jnp.ones((8, LANES), jnp.bfloat16)
    lying = lax.dot_general(
        ones, rows_ref[:, 768:], contract_last, preferred_element_type=jnp.float32
    )[:1, :]
    scores = []
    for i in range(total // tile):
        here = slice(i * tile, (i + 1) * tile)
        queries = [rows_ref[here, h * 128 : (h + 1) * 128] for h in range(heads)]
        scores.append(
            lax.dot_general(
                jnp.concatenate(queries, axis=0),
                rows_ref[: (i + 1) * tile, 512:640],
                contract_last,
                preferred_element_type=jnp.float32,
            )
        )
    for i in range(total // tile):
        seen = (i + 1) * tile
        here = slice(i * tile, seen)
        upright = rows_ref[here, 768:769].astype(jnp.float32) * float(LANES)
        row = lax.broadcasted_iota(jnp.int32, (tile, seen), 0) + i * tile
        column = lax.broadcasted_iota(jnp.int32, (tile, seen), 1)
        allowed = (column <= row) & (lying[:, :seen] == upright)
        bias = jnp.where(allowed, 0.0, -1e30)
        exponents = []
        for head in range(heads):
            masked = scores[i][head * tile : (head + 1) * tile] + bias
            row_max = jnp.max(masked, axis=-1, keepdims=True)
            exponents.append(jnp.exp2((masked - row_max) * factor).astype(jnp.bfloat16))
        values = rows_ref[:seen, 640:768]
        values = jnp.concatenate([values, jnp.ones_like(values)], axis=1)
        context = jnp.dot(
            jnp.concatenate(exponents, axis=0), values, preferred_element_type=jnp.float32
        )
        for head in range(heads):
            part = context[head * tile : (head + 1) * tile]
            result = part[:, :128] / part[:, 128:]
            out_ref[0, here, head * 128 : (head + 1) * 128] = result.astype(jnp.bfloat16)


def attend(where, early, blocks, weights, cosine, sine):
    rows = blocks[0].shape[0]
    total = cosine.shape[0]
    vmem = pl.BlockSpec(memory_space=VMEM)
    flops = 2 * 4 * rows * weights[0].shape[0] * 768
    return pl.pallas_call(
        functools.partial(attend_kernel, where),
        out_shape=jax.ShapeDtypeStruct((1, total, weights[0].shape[1]), jnp.bfloat16),
        in_specs=[vmem] * 10,
        out_specs=vmem,
        scratch_shapes=[pltpu.VMEM((total, 768 + LANES), jnp.bfloat16)],
        compiler_params=pltpu.CompilerParams(vmem_limit_bytes=20 << 20),
        cost_estimate=pl.CostEstimate(flops=flops, bytes_accessed=10 << 20, transcendentals=0),
    )(*early, *blocks, *weights, cosine, sine)


def routes(sections, group):
    def place(section, t):
        return section * group + t % group

    first, second, sibling = [], [], []
    for s in range(sections):
        for t in range(group):
            up = t % 2 == 0
            if s + 1 < sections:
                shift = (2 if up else 0) if s % 2 else (0 if up else -2)
                first.append((place(s, t), place(s + 1, t + shift)))
            second.append((place(s, t), place(s, t + (2 if up else -2))))
            sibling.append((place(s, t), place(s, t ^ 1)))
    return first, second, sibling


def per_device(sections, group, stash, slot, doc_ids, norm_gain, w_query, w_key, value_weight):
    first, second, sibling = routes(sections, group)
    weights = (w_query, w_key, value_weight)

    def go(block, route):
        return lax.ppermute(block, AXES, route)

    where = tuple(
        ((shift, True, swapped), (shift, False, swapped))
        for shift in (0, 1)
        for swapped in (False, True)
    )
    own = normalize(slot, stash, doc_ids, norm_gain)
    near_a = go(own, first)
    other = go(own, sibling)
    near_b = go(other, first)
    cosine, sine = tables(stash.shape[2] * group)
    far_a = go(near_a, second)
    near_c = go(near_a, sibling)
    rows_a = project(where[0], (near_a, near_c), weights, cosine, sine)
    far_b = go(near_b, second)
    near_d = go(near_b, sibling)
    rows_b = project(where[1], (near_b, near_d), weights, cosine, sine)
    far_c = go(far_a, sibling)
    rows_c = project(where[2], (far_a, far_c), weights, cosine, sine)
    far_d = go(far_b, sibling)
    early = (rows_a, rows_b, rows_c)
    return attend(where, early, (far_b, far_d), weights, cosine, sine)


def solution(mesh):
    placed = (
        P("section", None, "tp", None),
        P("section"),
        P("section", None, "tp"),
        P(),
        P(None, "tp"),
        P(None, "tp"),
        P(None, "tp"),
    )
    return jax.shard_map(
        functools.partial(per_device, mesh.shape["section"], mesh.shape["tp"]),
        mesh=mesh,
        in_specs=placed,
        out_specs=P("section", None, "tp"),
        check_vma=False,
    )
```

```python
import functools
import math

import jax
import jax.numpy as jnp
import numpy as np
from jax import lax
from jax.experimental import pallas as pl
from jax.experimental.pallas import tpu as pltpu
from jax.sharding import PartitionSpec as P

HEAD_SIZE = 128
LANES = 128
ROPE_BASE = 500000.0
NORM_EPSILON = 1e-05
AXES = ("section", "tp")
VMEM = pltpu.MemorySpace.VMEM


def fetch(source, target, sem):
    return pltpu.make_async_copy(source, target, sem)


def stay(x):
    return pltpu.with_memory_space_constraint(x, pltpu.MemorySpace.HBM)


def normalize_kernel(
    slot_ref, stash_ref, doc_ref, gain_ref, out_ref, low, high, docs, gain_buf, buf, sems
):
    rows, width = buf.shape
    pieces = sems.shape[0] - 2
    step = rows // pieces
    pick = slot_ref[0]
    copies = [
        fetch(doc_ref, docs, sems.at[0]),
        fetch(gain_ref, gain_buf, sems.at[1]),
    ]
    for i in range(pieces):
        part = pl.ds(i * step, step)
        copies.append(fetch(stash_ref.at[0, pick, part], buf.at[part], sems.at[2 + i]))
    for copy in copies:
        copy.start()
    for copy in copies[:2]:
        copy.wait()
    numbers = docs[0, pl.ds(pick, 1), :].astype(jnp.float32)
    row = lax.broadcasted_iota(jnp.int32, (rows, rows), 0)
    column = lax.broadcasted_iota(jnp.int32, (rows, rows), 1)
    upright = jnp.sum(jnp.where(row == column, numbers, 0.0), axis=1, keepdims=True)
    upright = jnp.broadcast_to(upright, (rows, LANES)).astype(jnp.bfloat16)
    out_ref[:, width:] = upright
    low[:, width:] = upright[: rows // 2]
    high[:, width:] = upright[rows // 2 :]
    gain = gain_buf[...].astype(jnp.float32)
    for i in range(pieces):
        copies[2 + i].wait()
        part = slice(i * step, (i + 1) * step)
        x = buf[part, :].astype(jnp.float32)
        scale = lax.rsqrt(jnp.mean(x * x, axis=-1, keepdims=True) + NORM_EPSILON)
        for j in range(width // LANES):
            lanes = slice(j * LANES, (j + 1) * LANES)
            scaled = (x[:, lanes] * scale * gain[j : j + 1, :]).astype(jnp.bfloat16)
            out_ref[part, lanes] = scaled
            first = i * step % (rows // 2)
            piece = low if i < pieces // 2 else high
            piece[first : first + step, lanes] = scaled


def normalize(slot, stash, doc_ids, gain):
    rows, width = stash.shape[2:]
    pieces = 4
    hbm = pl.BlockSpec(memory_space=pltpu.MemorySpace.HBM)

    return pl.pallas_call(
        normalize_kernel,
        out_shape=[
            jax.ShapeDtypeStruct((count, width + LANES), jnp.bfloat16)
            for count in (rows, rows // 2, rows // 2)
        ],
        in_specs=[pl.BlockSpec(memory_space=pltpu.MemorySpace.SMEM)] + [hbm] * 3,
        out_specs=[pl.BlockSpec(memory_space=VMEM)] * 3,
        scratch_shapes=[
            pltpu.VMEM(doc_ids.shape, doc_ids.dtype),
            pltpu.VMEM((width // LANES, LANES), gain.dtype),
            pltpu.VMEM((rows, width), jnp.bfloat16),
            pltpu.SemaphoreType.DMA((2 + pieces,)),
        ],
        compiler_params=pltpu.CompilerParams(vmem_limit_bytes=8 << 20),
    )(slot, stay(stash), stay(doc_ids), stay(gain.reshape(-1, LANES)))


def prepare_kernel(inverse_ref, w_query, w_key, w_value, cosine, sine, weights, sems):
    start, copies = 0, []
    for index, part in enumerate((w_query, w_key, w_value)):
        columns = part.shape[1]
        copies.append(fetch(part, weights.at[:, pl.ds(start, columns)], sems.at[index]))
        start += columns
    for copy in copies:
        copy.start()
    rows = cosine.shape[0]
    position = lax.broadcasted_iota(jnp.int32, (rows, LANES), 0).astype(jnp.float32)
    lane = lax.broadcasted_iota(jnp.int32, (rows, LANES), 1)
    angle = position * inverse_ref[...]
    cosine[...] = jnp.cos(angle)
    turned = jnp.sin(angle)
    sine[...] = jnp.where(lane < HEAD_SIZE // 2, -turned, turned)
    for copy in copies:
        copy.wait()


def prepare(total, w_query, w_key, w_value):
    exponent = -2.0 * np.arange(HEAD_SIZE // 2) / HEAD_SIZE
    inverse = np.tile(ROPE_BASE**exponent, 2)[None].astype(np.float32)
    parts = (w_query, w_key, w_value)
    vmem = pl.BlockSpec(memory_space=VMEM)
    hbm = pl.BlockSpec(memory_space=pltpu.MemorySpace.HBM)
    shape = jax.ShapeDtypeStruct((total, LANES), jnp.float32)
    columns = sum(part.shape[1] for part in parts)
    return pl.pallas_call(
        prepare_kernel,
        out_shape=(
            shape,
            shape,
            jax.ShapeDtypeStruct((w_query.shape[0], columns), w_query.dtype),
        ),
        in_specs=[vmem] + [hbm] * 3,
        out_specs=(vmem,) * 3,
        scratch_shapes=[pltpu.SemaphoreType.DMA((3,))],
        compiler_params=pltpu.CompilerParams(vmem_limit_bytes=10 << 20),
        cost_estimate=pl.CostEstimate(flops=4 << 20, bytes_accessed=8 << 20, transcendentals=0),
    )(inverse, *[stay(part) for part in parts])


def granule(chip_shift, mine, swapped):
    t, odd = lax.axis_index("tp"), 1 - lax.axis_index("section") % 2
    core, chips = t % 2, lax.axis_size("tp") // 2
    up = core if mine else 1 - core
    chip = lax.rem(t // 2 - odd + chips + jnp.where(up == 0, -chip_shift, 1 + chip_shift), chips)
    return 2 * chip + (1 - up if swapped else up)


def row_of(place, rows):
    return pl.multiple_of(granule(*place[:3]) * rows + place[3], 16)


def project_to(blocks, places, weights, cosine, sine, rows, store):
    width = weights.shape[0]
    x = jnp.concatenate([block[:, :width] for block in blocks], axis=0)
    numbers = jnp.concatenate([block[:, width:] for block in blocks], axis=0)
    products = [
        jnp.dot(x, weights[:, start : start + 256], preferred_element_type=jnp.float32)
        for start in range(0, 768, 256)
    ]
    first = 0
    for place in places:
        count, position = place[4], row_of(place, rows)
        here = slice(first, first + count)
        cos, sin = cosine[pl.ds(position, count), :], sine[pl.ds(position, count), :]
        for head in range(6):
            values = products[head // 2][here, (head % 2) * 128 : (head % 2) * 128 + 128]
            if head < 5:
                values = values * cos + pltpu.roll(values, 64, 1) * sin
            store(here, pl.ds(position, count), head * 128, values.astype(jnp.bfloat16))
        store(here, pl.ds(position, count), 768, numbers[here])
        first += count


def project_kernel(places, rows, b0, b1, weights, cosine, sine, out_ref):
    def store(here, there, column, values):
        out_ref[here, column : column + 128] = values

    project_to((b0, b1), places, weights, cosine, sine, rows, store)


def project(places, rows, blocks, weights, cosine, sine):
    count = sum(place[4] for place in places)
    vmem = pl.BlockSpec(memory_space=VMEM)
    flops = 2 * count * weights.shape[0] * 768
    return pl.pallas_call(
        functools.partial(project_kernel, places, rows),
        out_shape=jax.ShapeDtypeStruct((count, 768 + LANES), jnp.bfloat16),
        in_specs=[vmem] * 5,
        out_specs=vmem,
        compiler_params=pltpu.CompilerParams(vmem_limit_bytes=16 << 20),
        cost_estimate=pl.CostEstimate(flops=flops, bytes_accessed=8 << 20, transcendentals=0),
    )(*blocks, weights, cosine, sine)


def attend_kernel(
    near, far, last, rows, e0, e1, b0, b1, weights, cosine, sine, out_ref, rows_ref
):
    def store(here, there, column, values):
        rows_ref[there, column : column + 128] = values

    for places, early in ((near, e0), (far, e1)):
        first = 0
        for place in places:
            count = place[4]
            rows_ref[pl.ds(row_of(place, rows), count), :] = early[first : first + count, :]
            first += count
    project_to((b0, b1), last, weights, cosine, sine, rows, store)

    total = rows_ref.shape[0]
    heads, tile = 4, 128
    factor = math.log2(math.e) / math.sqrt(HEAD_SIZE)
    contract_last = (((1,), (1,)), ((), ()))
    ones = jnp.ones((8, LANES), jnp.bfloat16)
    lying = lax.dot_general(
        ones, rows_ref[:, 768:], contract_last, preferred_element_type=jnp.float32
    )[:1, :]
    scores = []
    for i in range(total // tile):
        here = slice(i * tile, (i + 1) * tile)
        queries = [rows_ref[here, h * 128 : (h + 1) * 128] for h in range(heads)]
        scores.append(
            lax.dot_general(
                jnp.concatenate(queries, axis=0),
                rows_ref[: (i + 1) * tile, 512:640],
                contract_last,
                preferred_element_type=jnp.float32,
            )
        )
    for i in range(total // tile):
        seen = (i + 1) * tile
        here = slice(i * tile, seen)
        upright = rows_ref[here, 768:769].astype(jnp.float32) * float(LANES)
        row = lax.broadcasted_iota(jnp.int32, (tile, seen), 0) + i * tile
        column = lax.broadcasted_iota(jnp.int32, (tile, seen), 1)
        allowed = (column <= row) & (lying[:, :seen] == upright)
        bias = jnp.where(allowed, 0.0, -1e30)
        exponents = []
        for head in range(heads):
            masked = scores[i][head * tile : (head + 1) * tile] + bias
            row_max = jnp.max(masked, axis=-1, keepdims=True)
            exponents.append(jnp.exp2((masked - row_max) * factor).astype(jnp.bfloat16))
        values = rows_ref[:seen, 640:768]
        values = jnp.concatenate([values, jnp.ones_like(values)], axis=1)
        context = jnp.dot(
            jnp.concatenate(exponents, axis=0), values, preferred_element_type=jnp.float32
        )
        for head in range(heads):
            part = context[head * tile : (head + 1) * tile]
            result = part[:, :128] / part[:, 128:]
            out_ref[0, here, head * 128 : (head + 1) * 128] = result.astype(jnp.bfloat16)


def attend(near, far, last, rows, early, blocks, weights, cosine, sine):
    total = cosine.shape[0]
    vmem = pl.BlockSpec(memory_space=VMEM)
    flops = 4 * total * total * 512
    return pl.pallas_call(
        functools.partial(attend_kernel, near, far, last, rows),
        out_shape=jax.ShapeDtypeStruct((1, total, 512), jnp.bfloat16),
        in_specs=[vmem] * 7,
        out_specs=vmem,
        scratch_shapes=[pltpu.VMEM((total, 768 + LANES), jnp.bfloat16)],
        compiler_params=pltpu.CompilerParams(vmem_limit_bytes=20 << 20),
        cost_estimate=pl.CostEstimate(flops=flops, bytes_accessed=10 << 20, transcendentals=0),
    )(*early, *blocks, weights, cosine, sine)


def join_kernel(*refs):
    first = 0
    for block in refs[:-1]:
        count = block.shape[0]
        refs[-1][first : first + count, :] = block[...]
        first += count


def join(*blocks):
    vmem = pl.BlockSpec(memory_space=VMEM)
    rows, width = sum(block.shape[0] for block in blocks), blocks[0].shape[1]
    return pl.pallas_call(
        join_kernel,
        out_shape=jax.ShapeDtypeStruct((rows, width), blocks[0].dtype),
        in_specs=[vmem] * len(blocks),
        out_specs=vmem,
        compiler_params=pltpu.CompilerParams(vmem_limit_bytes=6 << 20),
        cost_estimate=pl.CostEstimate(flops=1 << 20, bytes_accessed=1 << 20, transcendentals=0),
    )(*blocks)


def routes(sections, group):
    def place(section, t):
        return section * group + t % group

    first, second, sibling = [], [], []
    for s in range(sections):
        for t in range(group):
            up = t % 2 == 0
            if s + 1 < sections:
                shift = (2 if up else 0) if s % 2 else (0 if up else -2)
                first.append((place(s, t), place(s + 1, t + shift)))
            second.append((place(s, t), place(s, t + (2 if up else -2))))
            sibling.append((place(s, t), place(s, t ^ 1)))
    return first, second, sibling


def per_device(sections, group, stash, slot, doc_ids, norm_gain, w_query, w_key, value_weight):
    first, second, sibling = routes(sections, group)

    def go(block, route):
        return lax.ppermute(block, AXES, route)

    rows = stash.shape[2]

    def places(shift, parts):
        return [(shift, mine, *part) for mine in (True, False) for part in parts]

    near_places = places(0, [(False, 0, rows), (True, 0, rows)])
    far_places = places(1, [(False, 0, rows)])
    last_places = places(1, [(True, 0, rows)])
    own, low, high = normalize(slot, stash, doc_ids, norm_gain)
    near_a = go(low, first)
    near_b = go(high, first)
    other = go(own, sibling)
    near_c = go(other, first)
    cosine, sine, weights = prepare(rows * group, w_query, w_key, value_weight)
    far_a = go(near_a, second)
    far_b = go(near_b, second)
    far_c = go(near_c, second)
    near = join(near_a, near_b, near_c)
    near_other = go(near, sibling)
    far = join(far_a, far_b)
    far_other = go(far, sibling)
    rows_near = project(near_places, rows, (near, near_other), weights, cosine, sine)
    rows_far = project(far_places, rows, (far, far_other), weights, cosine, sine)
    last_other = go(far_c, sibling)
    return attend(
        near_places,
        far_places,
        last_places,
        rows,
        (rows_near, rows_far),
        (far_c, last_other),
        weights,
        cosine,
        sine,
    )


def solution(mesh):
    placed = (
        P("section", None, "tp", None),
        P("section"),
        P("section", None, "tp"),
        P(),
        P(None, "tp"),
        P(None, "tp"),
        P(None, "tp"),
    )
    return jax.shard_map(
        functools.partial(per_device, mesh.shape["section"], mesh.shape["tp"]),
        mesh=mesh,
        in_specs=placed,
        out_specs=P("section", None, "tp"),
        check_vma=False,
    )
```
